32 devices in a mesh: expert: 8 (over z, x), rep: 4 (over y, core).
Axes of the slice: x: 2, y: 2, z: 4, core: 2. Of those that a mesh axis runs over, the one named last changes fastest.
Arguments:
- features: bfloat16 [4096, 1024], P(('expert', 'rep')), may hold values from -20 to 20
- readout: bfloat16 [4096, 1024], P(('expert', 'rep')), may hold values from -20 to 20
- up_weight: bfloat16 [8, 1024, 2048], P('expert'), may hold values from -0.1875 to 0.1875
- down_weight: bfloat16 [8, 2048, 1024], P('expert'), may hold values from -0.125 to 0.125
- expert_ids: int32 [4096, 2], P(('expert', 'rep')), may hold values from 0 to 7, all different within a row; in each aligned block of 128 rows (0 to 127, 128 to 255, ...) at most 36 rows name the same one
- gate_values: float32 [4096, 2], P(('expert', 'rep')), may hold values from 0.2 to 1
Outputs:
- grad_up: bfloat16 [8, 1024, 2048], P('expert', 'rep')
- input_grad: float32 [4096, 1024], P(('expert', 'rep'))
- penalty: float32 [], replicated
The draws below stay inside these ranges and needn't reach their ends.
Inputs may be any that keep to these rules, and one draw needn't show every extreme that they name: `expert_ids`: each row names 2 different experts. In each aligned block of 128 rows (the rows of one device) no expert is named more than 36 times, a bound that some block reaches.
All inputs are finite; a program needn't handle non-finite values.
Results may differ from the reference program's by a relative error of at most 0.01.
Values may be sent and summed in bfloat16 or wider, within the bound.
No kernel may reach another device: no remote copies, remote signals or barrier semaphores. Data moves between devices by JAX's collectives and lax.ppermute only.
A program may use at most 128 MiB of HBM per device.

```python
import math
import jax
import jax.numpy as jnp
import numpy as np
from jax import lax

D = 1024
FF = 2048
TOPK = 2
TOK_DEV = 128
EXPERTS = 8
TOKENS = 4096
CAP = 36
N_EXPERT = 8
N_REP = 4


def draw_features(key, part):
    key_base, key_scale = jax.random.split(jax.random.fold_in(key, 11), 2)
    rising = 3.0 ** (jnp.arange(TOKENS, dtype=jnp.float32) / (TOKENS - 1))
    baseline = jax.random.normal(key_base, (TOKENS, D), jnp.float32)
    row_scale = jax.random.uniform(key_scale, (TOKENS, 1), jnp.float32, 0.7, 1.3)
    return jnp.clip(baseline * row_scale * rising[:, None], -20.0, 20.0).astype(jnp.bfloat16)


def draw_readout(key, part):
    key_base, key_scale = jax.random.split(jax.random.fold_in(key, 23), 2)
    rising = 3.0 ** (jnp.arange(TOKENS, dtype=jnp.float32) / (TOKENS - 1))
    baseline = jax.random.normal(key_base, (TOKENS, D), jnp.float32)
    row_scale = jax.random.uniform(key_scale, (TOKENS, 1), jnp.float32, 0.7, 1.3)
    return jnp.clip(baseline * row_scale * rising[:, None], -20.0, 20.0).astype(jnp.bfloat16)


def block_levels(rng, shape, pieces, low, high):
    level = 1.0
    for dim, parts in pieces:
        heights = jax.random.uniform(jax.random.fold_in(jax.random.fold_in(rng, 6), dim), (parts,), jnp.float32, low / len(pieces), high / len(pieces))
        level = level * jnp.repeat(jnp.exp(heights), shape[dim] // parts).reshape((-1,) + (1,) * (len(shape) - 1 - dim))
    return level


def shared_out(stream_key, own, number, rows, amount, top, most, slope):
    sequence = jax.random.permutation(stream_key, amount)
    packed, ordinary = portions_of(amount, rows * top, most, slope, True), portions_of(amount, rows * top, most, slope, False)
    places = jnp.arange(amount)

    def named(tallies, offset_by):
        used = int((tallies > 0).sum())
        fixed = max(1, used // 4)
        passed = fixed + (places - fixed + offset_by * (used - fixed)) % max(1, amount - fixed)
        return jnp.zeros((amount,), jnp.int32).at[sequence[jnp.where(places < fixed, places, passed)]].set(jnp.asarray(tallies, jnp.int32))

    tallies = jnp.where(number % 4 == 0, named(packed, number // 4), named(ordinary, number - number // 4 - 1))
    mixed = jax.random.permutation(jax.random.fold_in(own, 3), amount)
    donor, sink = mixed[0:amount // 2 * 2:2], mixed[1:amount // 2 * 2:2]
    margin = jnp.minimum(tallies[donor] - 1, most - tallies[sink]) // 2
    margin = jnp.where((donor == sequence[0]) | (sink == sequence[0]) | (tallies[sink] == 0), 0, jnp.maximum(margin, 0))
    passed = jax.random.randint(jax.random.fold_in(own, 4), (amount // 2,), 0, 1 << 20) % (margin + 1)
    tallies = tallies.at[donor].add(-passed).at[sink].add(passed)
    labels = jnp.searchsorted(jnp.cumsum(tallies), jnp.arange(rows * top), side="right").astype(jnp.int32)
    table = labels.reshape(top, rows).T
    table = table[jax.random.permutation(jax.random.fold_in(own, 1), rows)]
    offset_by = jax.random.randint(jax.random.fold_in(own, 2), (rows, 1), 0, top)
    return jnp.take_along_axis(table, (jnp.arange(top)[None, :] + offset_by) % top, axis=1)


def portions_of(amount, total, limit, skew, full):
    portions = [(1 << 20) // math.isqrt(grade ** skew) + 1 for grade in range(1, amount + 1)]
    largest = limit if full else min(limit, max(-(-total // amount), total * portions[0] // sum(portions)))
    least = 1 if total - largest >= amount - 1 else 0
    counts, rest = [largest] + [least] * (amount - 1), total - largest - least * (amount - 1)
    while rest > 0:
        candidates = [i for i in range(1, amount) if counts[i] < largest] or [i for i in range(1, amount) if counts[i] < limit]
        mass, left = sum([portions[i] for i in candidates]), rest
        for i in candidates:
            extra = min(limit - counts[i], max(1, left * portions[i] // mass), rest)
            counts[i] = counts[i] + extra
            rest = rest - extra
    return np.array(counts)


def gaussian(stream_key, extent, width, most, shards=(), kind=jnp.bfloat16):
    drawn = width * jax.random.normal(stream_key, extent, jnp.float32)
    if shards:
        drawn = drawn * block_levels(stream_key, extent, shards, -0.22, 0.18)
    return jnp.clip(drawn, -most, most).astype(kind)


def setup_inputs(seed: int = 0) -> dict:
    key_of = jax.random.split(jax.random.key(seed), 7)
    features = draw_features(jax.random.fold_in(key_of[6], 71), 0)
    readout = draw_readout(jax.random.fold_in(key_of[6], 71), 0)
    up_weight = gaussian(key_of[2], (EXPERTS, D, FF), D ** -0.5, 0.1875, ((0, 8),))
    down_weight = gaussian(key_of[3], (EXPERTS, FF, D), FF ** -0.5, 0.125, ((0, 8),))
    expert_ids_keys = jax.random.split(jax.random.fold_in(key_of[4], 1), TOKENS // TOK_DEV)
    expert_ids_turns = jax.random.permutation(jax.random.fold_in(key_of[4], 3), TOKENS // TOK_DEV)
    expert_ids = jax.vmap(lambda own, number: shared_out(jax.random.fold_in(key_of[4], 2), own, number, TOK_DEV, EXPERTS, TOPK, CAP, 1))(expert_ids_keys, expert_ids_turns).reshape((TOKENS, TOPK))
    gate_values = jnp.clip(0.2 + 0.8 * jax.random.uniform(key_of[5], (TOKENS, TOPK), jnp.float32) ** block_levels(key_of[5], (TOKENS, TOPK), ((0, 32),), -0.2, 0.2), 0.2, 1.0)
    return {"features": features, "readout": readout, "up_weight": up_weight, "down_weight": down_weight, "expert_ids": expert_ids, "gate_values": gate_values}


def silu_slopes(pre_act):
    logistic = jax.nn.sigmoid(pre_act)
    first = logistic * (1.0 + pre_act * (1.0 - logistic))
    second = logistic * (1.0 - logistic) * (2.0 + pre_act * (1.0 - 2.0 * logistic))
    return first, second


def contract_last(left, right):
    return lax.dot_general(left, right, (((1,), (1,)), ((), ())), preferred_element_type=jnp.float32)


def expert_hidden(slot_x, slot_r, up_matrix, down_matrix):
    pre_act = jnp.dot(slot_x, up_matrix, preferred_element_type=jnp.float32)
    projected = jnp.dot(slot_r, down_matrix.T, preferred_element_type=jnp.float32)
    first, second = silu_slopes(pre_act)
    scaled = (first * projected).astype(jnp.bfloat16)
    return scaled, pre_act, projected


def by_copy(values):
    cols = values.shape[1]
    shaped = values.reshape(N_EXPERT, N_REP, CAP, cols).transpose(1, 0, 2, 3)
    return shaped.reshape(N_REP, N_EXPERT * CAP, cols).astype(jnp.float32)


def reference(features, readout, up_weight, down_weight, expert_ids, gate_values):
    tokens_all = features.shape[0]
    blocks = tokens_all // TOK_DEV
    block_ids = expert_ids.reshape(blocks, 2 * TOK_DEV)
    onehot = (block_ids[:, :, None] == jnp.arange(EXPERTS, dtype=jnp.int32)[None, None, :]).astype(jnp.int32)
    earlier = jnp.cumsum(onehot, axis=1) - onehot
    slot_index = jnp.sum(earlier * onehot, axis=2).astype(jnp.int32)
    position = (jnp.arange(blocks, dtype=jnp.int32)[:, None] * CAP + slot_index).reshape(-1).astype(jnp.int32)
    flat_ids = expert_ids.reshape(-1).astype(jnp.int32)
    pair_count = 2 * tokens_all
    table = jnp.full((EXPERTS, blocks * CAP), pair_count, jnp.int32)
    table = table.at[flat_ids, position].set(jnp.arange(pair_count, dtype=jnp.int32))
    zero_row = jnp.zeros((1, D), jnp.bfloat16)
    padded_x = jnp.concatenate([features, zero_row], axis=0)
    padded_r = jnp.concatenate([readout, zero_row], axis=0)

    def gather_slots(table_row):
        token_index = (table_row // 2).astype(jnp.int32)
        return padded_x[token_index], padded_r[token_index]

    def forward(operands):
        up_matrix, down_matrix, table_row = operands
        slot_x, slot_r = gather_slots(table_row)
        scaled, pre_act, projected = expert_hidden(slot_x, slot_r, up_matrix, down_matrix)
        return contract_last(scaled, up_matrix).astype(jnp.bfloat16)

    outputs = lax.map(forward, (up_weight, down_weight, table))
    pair_out = outputs[flat_ids, position].astype(jnp.float32).reshape(tokens_all, 2, D)
    input_grad = readout.astype(jnp.float32) + gate_values[:, 0:1] * pair_out[:, 0] + gate_values[:, 1:2] * pair_out[:, 1]
    penalty = jnp.sum(input_grad * input_grad) / (2.0 * tokens_all * D)
    cotangent = (gate_values[:, :, None] * input_grad[:, None, :]).reshape(pair_count, D).astype(jnp.bfloat16)
    padded_w = jnp.concatenate([cotangent, zero_row], axis=0)

    def backward(operands):
        up_matrix, down_matrix, table_row = operands
        slot_x, slot_r = gather_slots(table_row)
        slot_w = padded_w[table_row]
        scaled, pre_act, projected = expert_hidden(slot_x, slot_r, up_matrix, down_matrix)
        first, second = silu_slopes(pre_act)
        slope_grad = jnp.dot(slot_w, up_matrix, preferred_element_type=jnp.float32)
        pre_grad = (slope_grad * projected * second).astype(jnp.bfloat16)
        term = jnp.einsum("rsd,rsf->rdf", by_copy(slot_w), by_copy(scaled))
        term = term + jnp.einsum("rsd,rsf->rdf", by_copy(slot_x), by_copy(pre_grad))
        rounded = lax.optimization_barrier(term.astype(jnp.bfloat16)).astype(jnp.float32)
        return jnp.sum(rounded, axis=0).astype(jnp.bfloat16)

    grad_up = lax.map(backward, (up_weight, down_weight, table))
    return grad_up, input_grad, penalty
```

```python
import functools

import jax
import jax.numpy as jnp
from jax import lax
from jax.experimental import pallas as pl
from jax.experimental.pallas import tpu as pltpu
from jax.sharding import PartitionSpec as P


F32 = jnp.float32
BF16 = jnp.bfloat16
VMEM = pl.BlockSpec(memory_space=pltpu.VMEM)
SMEM = pl.BlockSpec(memory_space=pltpu.SMEM)
MIB = 1 << 20
DIRECT_PEERS = 8


def round_up(value, step):
    return (value + step - 1) // step * step


def dot(left, right, dims):
    return lax.dot_general(left, right, ((dims[:1], dims[1:]), ((), ())), preferred_element_type=F32)


def block_of(refs, index):
    return refs[index] if len(refs) > 1 else refs[0].at[index]


def peers_of(shape, base):
    return lax.broadcasted_iota(jnp.int32, shape, 0) ^ base


def pack_kernel(experts, capacity, n_out, base_ref, ids_ref, x_ref, r_ref, rank_ref, *out_refs):
    tokens = x_ref.shape[0]
    peer = peers_of((experts, tokens), base_ref[0])
    named = (ids_ref[0:1, :] == peer) | (ids_ref[1:2, :] == peer)
    row = lax.broadcasted_iota(jnp.int32, (tokens, tokens), 0)
    col = lax.broadcasted_iota(jnp.int32, (tokens, tokens), 1)
    before = jnp.where(row < col, 1.0, 0.0).astype(BF16)
    rank = dot(jnp.where(named, 1.0, 0.0).astype(BF16), before, (1, 0))
    rank_x = jnp.where(named, rank, -1.0).astype(jnp.int32)
    rank_r = jnp.where(named, rank + capacity, -1.0).astype(jnp.int32)
    rank_ref[...] = rank_x
    both = jnp.concatenate([rank_x, rank_r], axis=1)
    stride = round_up(2 * capacity, 8)
    slot = lax.broadcasted_iota(jnp.int32, (stride, 2 * tokens), 0)
    placing = jnp.concatenate(
        [jnp.where(slot == both[e : e + 1, :], 1.0, 0.0) for e in range(experts)], axis=0
    ).astype(BF16)
    rows = jnp.concatenate([x_ref[...], r_ref[...]], axis=0)
    packed = dot(placing, rows, (1, 0))
    for e in range(experts):
        block_of(out_refs, e)[...] = packed[e * stride : e * stride + 2 * capacity].astype(BF16)


def place_kernel(experts, stride, base_ref, ids_ref, rank_ref, out_ref, flip_ref):
    tokens = ids_ref.shape[1]
    peer = peers_of((experts, tokens), base_ref[0])
    rank = rank_ref[...]
    both = jnp.concatenate(
        [jnp.where(ids_ref[k : k + 1, :] == peer, rank, -1) for k in range(2)], axis=1
    )
    slot = lax.broadcasted_iota(jnp.int32, (stride, 2 * tokens), 0)
    placing = jnp.concatenate(
        [jnp.where(slot == both[e : e + 1, :], 1.0, 0.0) for e in range(experts)], axis=0
    )
    out_ref[...] = placing.astype(BF16)
    flip_ref[...] = placing.T.astype(BF16)


def expert_kernel(experts, capacity, stride, n_in, with_back, *refs):
    in_refs, (up_ref, down_ref), refs = refs[:n_in], refs[n_in : n_in + 2], refs[n_in + 2 :]
    scaled_ref, pc_ref, x_ref, refs = refs[0], refs[1], refs[2], refs[3:]
    r_ref = refs[-2] if with_back else refs[-1]
    step = pl.program_id(0)

    @pl.when(step == 0)
    def _():
        pad = jnp.zeros((stride - capacity, x_ref.shape[1]), F32)
        for e in range(experts):
            block = block_of(in_refs, e)[...].astype(F32)
            where = pl.ds(e * stride, stride)
            x_ref[where, :] = jnp.concatenate([block[:capacity], pad], axis=0).astype(BF16)
            r_ref[where, :] = jnp.concatenate([block[capacity:], pad], axis=0).astype(BF16)

    pre = dot(x_ref[...], up_ref[...], (1, 0))
    proj = dot(r_ref[...], down_ref[...], (1, 1))
    gate = 1.0 / (1.0 + jnp.exp(-pre))
    rest = 1.0 - gate
    slope = gate * (1.0 + pre * rest)
    curve = gate * rest * (2.0 + pre * (1.0 - 2.0 * gate))
    scaled = (slope * proj).astype(BF16)
    scaled_ref[...] = scaled
    pc_ref[...] = proj * curve
    if with_back:
        back_refs, acc_ref = refs[:-2], refs[-1]
        term = dot(scaled, up_ref[...], (1, 1))

        @pl.when(step == 0)
        def _():
            acc_ref[...] = term

        @pl.when(step > 0)
        def _():
            acc_ref[...] += term

        @pl.when(step == pl.num_programs(0) - 1)
        def _():
            for e in range(experts):
                block_of(back_refs, e)[...] = acc_ref[pl.ds(e * stride, stride), :].astype(BF16)


def combine_kernel(experts, stride, n_in, *refs):
    in_refs, refs = refs[:n_in], refs[n_in:]
    place_ref, flip_ref, gate_ref, r_ref, grad_ref, square_ref, *out_refs = refs
    tokens = r_ref.shape[0]
    rows = jnp.concatenate(
        [block_of(in_refs, e)[...].astype(F32) for e in range(experts)], axis=0
    ).astype(BF16)
    pairs = dot(flip_ref[...], rows, (1, 0))
    gate0, gate1 = gate_ref[:, 0:1], gate_ref[:, 1:2]
    grad = r_ref[...].astype(F32) + gate0 * pairs[:tokens] + gate1 * pairs[tokens:]
    grad_ref[...] = grad
    cot = jnp.concatenate([(gate0 * grad).astype(BF16), (gate1 * grad).astype(BF16)], axis=0)
    sent = dot(place_ref[...], cot, (1, 0))
    for e in range(experts):
        block_of(out_refs, e)[...] = sent[e * stride : (e + 1) * stride].astype(BF16)
    square_ref[...] = jnp.broadcast_to(jnp.sum(grad * grad), square_ref.shape)


def grad_kernel(experts, stride, n_in, parts, width, *refs):
    own_refs, far_refs, refs = refs[:n_in], refs[n_in : 2 * n_in], refs[2 * n_in :]
    at_ref, x0_ref, x1_ref, up_ref, s0_ref, s1_ref, p0_ref, p1_ref = refs[:8]
    out_refs, (cot_ref, cott_ref, xt_ref) = refs[8 : 8 + parts], refs[8 + parts :]
    half = experts * stride

    @pl.when(pl.program_id(0) == 0)
    def _():
        for side, side_refs in enumerate((own_refs, far_refs)):
            for e in range(experts):
                where = pl.ds(side * half + e * stride, stride)
                cot_ref[where, :] = block_of(side_refs, e)[...]
        for p in range(parts):
            lanes = pl.ds(pl.multiple_of(at_ref[p] * width, width), width)
            into = pl.ds(p * width, width)
            cott_ref[into, :] = cot_ref[:, lanes].T
            xt_ref[into, :half] = x0_ref[:, lanes].T
            xt_ref[into, half:] = x1_ref[:, lanes].T

    slope_grad = dot(cot_ref[...], up_ref[...], (1, 0))
    pre0 = (slope_grad[:half] * p0_ref[...]).astype(BF16)
    pre1 = (slope_grad[half:] * p1_ref[...]).astype(BF16)
    total = (
        dot(cott_ref[:, :half], s0_ref[...], (1, 0))
        + dot(cott_ref[:, half:], s1_ref[...], (1, 0))
        + dot(xt_ref[:, :half], pre0, (1, 0))
        + dot(xt_ref[:, half:], pre1, (1, 0))
    )
    for p in range(parts):
        out_refs[p][...] = total[p * width : (p + 1) * width].astype(out_refs[p].dtype)


def call(kernel, out_shape, vmem_mib, flops, bytes_accessed, name, **kwargs):
    return pl.pallas_call(
        kernel,
        out_shape=out_shape,
        compiler_params=pltpu.CompilerParams(vmem_limit_bytes=vmem_mib * MIB),
        cost_estimate=pl.CostEstimate(
            flops=flops, bytes_accessed=bytes_accessed, transcendentals=0
        ),
        name=name,
        **kwargs,
    )


def shift(array, axis, mask):
    size = lax.axis_size(axis)
    return lax.ppermute(array, axis, [(i, i ^ mask) for i in range(size)])


def exchange(blocks):
    if len(blocks) == 1:
        return [lax.all_to_all(blocks[0], "expert", split_axis=0, concat_axis=0, tiled=True)]
    got = {0: blocks[0]}
    for mask in sorted(range(1, len(blocks)), reverse=True):
        got[mask] = shift(blocks[mask], "expert", mask)
    return [got[mask] for mask in range(len(blocks))]


def body(features, readout, up_weight, down_weight, expert_ids, gate_values):
    tokens, width = features.shape
    hidden = up_weight.shape[2]
    groups, copies = lax.axis_size("expert"), lax.axis_size("rep")
    experts = groups * up_weight.shape[0]
    capacity = (9 * tokens * 2 + 8 * experts - 1) // (8 * experts)
    stride = round_up(capacity, 8)
    slots = experts * stride
    up, down = up_weight[0], down_weight[0]
    ids = expert_ids.T
    direct = experts <= DIRECT_PEERS
    here = lax.axis_index("expert").astype(jnp.int32)
    base = jnp.where(direct, here, 0).reshape(1)
    pieces = experts if direct else 1

    def blocks_shape(rows, dtype=BF16):
        if direct:
            return [jax.ShapeDtypeStruct((rows, width), dtype)] * experts
        return [jax.ShapeDtypeStruct((experts, rows, width), dtype)]

    rank, *sends = call(
        functools.partial(pack_kernel, experts, capacity, pieces),
        [jax.ShapeDtypeStruct((experts, tokens), jnp.int32)] + blocks_shape(2 * capacity),
        16, 4 * experts * capacity * 2 * tokens * width, 4 * tokens * width * 2, "pack",
        in_specs=[SMEM, VMEM, VMEM, VMEM],
        out_specs=[VMEM] * (1 + pieces),
    )(base, ids, features, readout)
    place, flip = call(
        functools.partial(place_kernel, experts, stride),
        [
            jax.ShapeDtypeStruct((slots, 2 * tokens), BF16),
            jax.ShapeDtypeStruct((2 * tokens, slots), BF16),
        ],
        8, 1 << 20, 1 << 18, "place",
        in_specs=[SMEM, VMEM, VMEM],
        out_specs=[VMEM] * 2,
    )(base, ids, rank)
    own = exchange(sends)
    far_mask = copies // 2
    far = [shift(block, "rep", far_mask) for block in own]

    tile = min(512, hidden)
    steps = hidden // tile
    whole = lambda shape: pl.BlockSpec(shape, lambda j: (0,) * len(shape))

    def run_expert(blocks, with_back):
        backs = blocks_shape(stride) if with_back else []
        outs = [
            jax.ShapeDtypeStruct((slots, hidden), BF16),
            jax.ShapeDtypeStruct((slots, hidden), F32),
            jax.ShapeDtypeStruct((slots, width), BF16),
        ] + backs
        scratch = [pltpu.VMEM((slots, width), BF16)]
        if with_back:
            scratch.append(pltpu.VMEM((slots, width), F32))
        return call(
            functools.partial(expert_kernel, experts, capacity, stride, pieces, with_back),
            outs, 24, (6 if with_back else 4) * slots * width * hidden,
            8 * width * hidden + 6 * slots * hidden, "expert",
            grid=(steps,),
            in_specs=[whole(b.shape) for b in blocks]
            + [
                pl.BlockSpec((width, tile), lambda j: (0, j)),
                pl.BlockSpec((tile, width), lambda j: (j, 0)),
            ],
            out_specs=[
                pl.BlockSpec((slots, tile), lambda j: (0, j)),
                pl.BlockSpec((slots, tile), lambda j: (0, j)),
                whole((slots, width)),
            ]
            + [whole(b.shape) for b in backs],
            scratch_shapes=scratch,
        )(*blocks, up, down)

    scaled0, pc0, x0, *backs = run_expert(own, True)
    returned = exchange(backs)
    scaled1, pc1, x1 = run_expert(far, False)

    input_grad, square, *cots = call(
        functools.partial(combine_kernel, experts, stride, pieces),
        [
            jax.ShapeDtypeStruct((tokens, width), F32),
            jax.ShapeDtypeStruct((8, 128), F32),
        ]
        + blocks_shape(stride),
        16, 8 * slots * tokens * width, 4 * slots * width + 6 * tokens * width, "combine",
        in_specs=[VMEM] * (pieces + 4),
        out_specs=[VMEM] * (2 + pieces),
    )(*returned, place, flip, gate_values, readout)
    cot_own = exchange(cots)
    cot_far = [shift(block, "rep", far_mask) for block in cot_own]

    mask = 1
    while mask < groups:
        square = square + shift(square, "expert", mask)
        mask *= 2
    mask = 1
    while mask < copies:
        square = square + shift(square, "rep", mask)
        mask *= 2
    penalty = square[0, 0] / (2.0 * tokens * groups * copies * width)

    parts = max(1, far_mask)
    part = width // copies
    me = lax.axis_index("rep").astype(jnp.int32)
    at = jnp.stack([me ^ p for p in range(parts)])
    grads = call(
        functools.partial(grad_kernel, experts, stride, pieces, parts, part),
        [jax.ShapeDtypeStruct((part, hidden), F32 if p == 0 else BF16) for p in range(parts)],
        32, 4 * slots * width * hidden + 8 * slots * parts * part * hidden,
        2 * width * hidden + 12 * slots * hidden, "grad",
        grid=(steps,),
        in_specs=[whole(b.shape) for b in cot_own + cot_far]
        + [
            SMEM,
            whole((slots, width)),
            whole((slots, width)),
            pl.BlockSpec((width, tile), lambda j: (0, j)),
        ]
        + [pl.BlockSpec((slots, tile), lambda j: (0, j))] * 4,
        out_specs=[pl.BlockSpec((part, tile), lambda j: (0, j))] * parts,
        scratch_shapes=[
            pltpu.VMEM((2 * slots, width), BF16),
            pltpu.VMEM((parts * part, 2 * slots), BF16),
            pltpu.VMEM((parts * part, 2 * slots), BF16),
        ],
    )(*cot_own, *cot_far, at, x0, x1, up, scaled0, scaled1, pc0, pc1)
    total = grads[0]
    for p in range(1, parts):
        total = total + shift(grads[p], "rep", p).astype(F32)
    return total.astype(BF16)[None], input_grad, penalty


def solution(mesh):
    both = P(("expert", "rep"), None)
    return jax.shard_map(
        body,
        mesh=mesh,
        in_specs=(both, both, P("expert", None, None), P("expert", None, None), both, both),
        out_specs=(P("expert", "rep", None), both, P()),
        check_vma=False,
    )
```

```python
import functools

import jax
import jax.numpy as jnp
from jax import lax
from jax.experimental import pallas as pl
from jax.experimental.pallas import tpu as pltpu
from jax.sharding import PartitionSpec as P


F32 = jnp.float32
BF16 = jnp.bfloat16
VMEM = pl.BlockSpec(memory_space=pltpu.VMEM)
SMEM = pl.BlockSpec(memory_space=pltpu.SMEM)
ANY = pl.BlockSpec(memory_space=pl.ANY)
MIB = 1 << 20
TILE = 512
DIRECT_PEERS = 8


def round_up(value, step):
    return (value + step - 1) // step * step


def dot(left, right, dims):
    return lax.dot_general(left, right, ((dims[:1], dims[1:]), ((), ())), preferred_element_type=F32)


def block_of(refs, index):
    return refs[index] if len(refs) > 1 else refs[0].at[index]


def peers_of(shape):
    block = lax.broadcasted_iota(jnp.int32, shape, 0)
    return block ^ lax.axis_index("expert") if shape[0] <= DIRECT_PEERS else block


def lanes_of(index, width):
    return pl.ds(pl.multiple_of((lax.axis_index("rep") ^ index) * width, width), width)


def pack_kernel(experts, capacity, ids_hbm, x_hbm, r_hbm, rank_ref, *refs):
    *out_refs, ids_ref, rows_ref, sems = refs
    tokens = x_hbm.shape[0]
    copies = [
        pltpu.make_async_copy(ids_hbm, ids_ref, sems.at[0]),
        pltpu.make_async_copy(x_hbm, rows_ref.at[pl.ds(0, tokens)], sems.at[1]),
        pltpu.make_async_copy(r_hbm, rows_ref.at[pl.ds(tokens, tokens)], sems.at[2]),
    ]
    for copy in copies:
        copy.start()
    copies[0].wait()
    peer = peers_of((experts, tokens))
    named = (ids_ref[0:1, :] == peer) | (ids_ref[1:2, :] == peer)
    row = lax.broadcasted_iota(jnp.int32, (tokens, tokens), 0)
    col = lax.broadcasted_iota(jnp.int32, (tokens, tokens), 1)
    before = jnp.where(row < col, 1.0, 0.0).astype(BF16)
    rank = dot(jnp.where(named, 1.0, 0.0).astype(BF16), before, (1, 0))
    rank_x = jnp.where(named, rank, -1.0).astype(jnp.int32)
    rank_r = jnp.where(named, rank + capacity, -1.0).astype(jnp.int32)
    rank_ref[...] = rank_x
    both = jnp.concatenate([rank_x, rank_r], axis=1)
    stride = round_up(2 * capacity, 8)
    slot = lax.broadcasted_iota(jnp.int32, (stride, 2 * tokens), 0)
    placing = jnp.concatenate(
        [jnp.where(slot == both[e : e + 1, :], 1.0, 0.0) for e in range(experts)], axis=0
    ).astype(BF16)
    for copy in copies[1:]:
        copy.wait()
    packed = dot(placing, rows_ref[...], (1, 0))
    for e in range(experts):
        block_of(out_refs, e)[...] = packed[e * stride : e * stride + 2 * capacity].astype(BF16)


def place_kernel(experts, stride, ids_ref, rank_ref, out_ref, flip_ref):
    tokens = ids_ref.shape[1]
    peer = peers_of((experts, tokens))
    rank = rank_ref[...]
    both = jnp.concatenate(
        [jnp.where(ids_ref[k : k + 1, :] == peer, rank, -1) for k in range(2)], axis=1
    )
    slot = lax.broadcasted_iota(jnp.int32, (stride, 2 * tokens), 0)
    placing = jnp.concatenate(
        [jnp.where(slot == both[e : e + 1, :], 1.0, 0.0) for e in range(experts)], axis=0
    )
    out_ref[...] = placing.astype(BF16)
    flip_ref[...] = placing.T.astype(BF16)


def fetch_kernel(up_hbm, down_hbm, up_ref, down_ref, sems):
    copies = [
        pltpu.make_async_copy(up_hbm, up_ref, sems.at[0]),
        pltpu.make_async_copy(down_hbm, down_ref, sems.at[1]),
    ]
    for copy in copies:
        copy.start()
    for copy in copies:
        copy.wait()


def gather_rows(in_refs, experts, capacity, stride, x_ref, r_ref):
    pad = jnp.zeros((stride - capacity, x_ref.shape[1]), F32)
    for e in range(experts):
        block = block_of(in_refs, e)[...].astype(F32)
        where = pl.ds(e * stride, stride)
        x_ref[where, :] = jnp.concatenate([block[:capacity], pad], axis=0).astype(BF16)
        r_ref[where, :] = jnp.concatenate([block[capacity:], pad], axis=0).astype(BF16)


def hidden_of(x, r, up_ref, down_ref, cols, scaled_ref, pc_ref):
    pre = dot(x, up_ref[:, cols], (1, 0))
    proj = dot(r, down_ref[cols, :], (1, 1))
    gate = 1.0 / (1.0 + jnp.exp(-pre))
    rest = 1.0 - gate
    slope = gate * (1.0 + pre * rest)
    curve = gate * rest * (2.0 + pre * (1.0 - 2.0 * gate))
    scaled = (slope * proj).astype(BF16)
    scaled_ref[:, cols] = scaled
    pc_ref[:, cols] = proj * curve
    return scaled


def tiles_of(hidden, tile):
    return [slice(at, at + tile) for at in range(0, hidden, tile)]


def own_kernel(experts, capacity, stride, tile, n_in, *refs):
    in_refs, (up_ref, down_ref), refs = refs[:n_in], refs[n_in : n_in + 2], refs[n_in + 2 :]
    scaled_ref, pc_ref, x_ref, *back_refs, r_ref = refs
    gather_rows(in_refs, experts, capacity, stride, x_ref, r_ref)
    x, r = x_ref[...], r_ref[...]
    back, late = None, None
    for cols in tiles_of(up_ref.shape[1], tile):
        scaled = hidden_of(x, r, up_ref, down_ref, cols, scaled_ref, pc_ref)
        if late is not None:
            term = dot(late[0], up_ref[:, late[1]], (1, 1))
            back = term if back is None else back + term
        late = scaled, cols
    term = dot(late[0], up_ref[:, late[1]], (1, 1))
    back = term if back is None else back + term
    for e in range(experts):
        block_of(back_refs, e)[...] = back[e * stride : (e + 1) * stride].astype(BF16)


def far_kernel(experts, capacity, stride, tile, n_in, parts, width, *refs):
    in_refs, refs = refs[:n_in], refs[n_in:]
    own_ref, up_ref, down_ref, scaled_ref, pc_ref, xt_ref, x_ref, r_ref = refs
    half = experts * stride
    gather_rows(in_refs, experts, capacity, stride, x_ref, r_ref)
    x, r = x_ref[...], r_ref[...]
    for cols in tiles_of(up_ref.shape[1], tile):
        hidden_of(x, r, up_ref, down_ref, cols, scaled_ref, pc_ref)
    for p in range(parts):
        lanes = lanes_of(p, width)
        xt_ref[p * width : (p + 1) * width, :half] = own_ref[:, lanes].T
        xt_ref[p * width : (p + 1) * width, half:] = x_ref[:, lanes].T


def combine_kernel(experts, capacity, stride, n_in, *refs):
    in_refs, refs = refs[:n_in], refs[n_in:]
    place_ref, flip_ref, gate_ref, r_ref, grad_ref, *out_refs = refs
    tokens = r_ref.shape[0]
    rows = jnp.concatenate(
        [block_of(in_refs, e)[...].astype(F32) for e in range(experts)], axis=0
    ).astype(BF16)
    pairs = dot(flip_ref[...], rows, (1, 0))
    gates = jnp.concatenate([gate_ref[...], jnp.zeros((6, tokens), F32)], axis=0).T
    gate0, gate1 = gates[:, 0:1], gates[:, 1:2]
    grad = r_ref[...].astype(F32) + gate0 * pairs[:tokens] + gate1 * pairs[tokens:]
    grad_ref[...] = grad
    cot = jnp.concatenate([(gate0 * grad).astype(BF16), (gate1 * grad).astype(BF16)], axis=0)
    sent = dot(place_ref[...], cot, (1, 0))
    square = jnp.full((stride, r_ref.shape[1]), jnp.sum(grad * grad), F32)
    high = square.astype(BF16).astype(F32)
    middle = (square - high).astype(BF16).astype(F32)
    lane = lax.broadcasted_iota(jnp.int32, square.shape, 1)
    row = lax.broadcasted_iota(jnp.int32, square.shape, 0)
    terms = jnp.where(lane < 128, high, jnp.where(lane < 256, middle, square - high - middle))
    for e in range(experts):
        block = jnp.where(row == capacity, terms, sent[e * stride : (e + 1) * stride])
        block_of(out_refs, e)[...] = block.astype(BF16)


def square_of(blocks, capacity):
    low = capacity // 8 * 8
    sums = []
    for block in blocks:
        row = block[low : low + 8, :384].astype(F32)[capacity - low : capacity - low + 1]
        sums.append(row[:, :128] + row[:, 128:256] + row[:, 256:])
    while len(sums) > 1:
        sums = [sums[i] + sums[i + 1] for i in range(0, len(sums), 2)]
    return sums[0]


def grad_kernel(experts, capacity, stride, tile, n_in, parts, width, *refs):
    own_refs, far_refs, refs = refs[:n_in], refs[n_in : 2 * n_in], refs[2 * n_in :]
    xt_ref, up_ref, s0_ref, s1_ref, p0_ref, p1_ref, square_ref = refs[:7]
    out_refs, (cot_ref, cott_ref) = refs[7 : 7 + parts], refs[7 + parts :]
    half = experts * stride
    square = jnp.zeros((1, 128), F32)
    for side, side_refs in enumerate((own_refs, far_refs)):
        blocks = [block_of(side_refs, e)[...] for e in range(experts)]
        square = square + square_of(blocks, capacity)
        for e in range(experts):
            cot_ref[side * half + e * stride : side * half + (e + 1) * stride, :] = blocks[e]
    square_ref[...] = jnp.broadcast_to(square, square_ref.shape)
    for p in range(parts):
        lanes = lanes_of(p, width)
        cott_ref[p * width : (p + 1) * width, :] = cot_ref[:, lanes].T
    cot = cot_ref[...]
    tiles = tiles_of(up_ref.shape[1], tile)
    slope_grad = dot(cot, up_ref[:, tiles[0]], (1, 0))
    for index, cols in enumerate(tiles):
        pre0 = (slope_grad[:half] * p0_ref[:, cols]).astype(BF16)
        pre1 = (slope_grad[half:] * p1_ref[:, cols]).astype(BF16)
        if index + 1 < len(tiles):
            slope_grad = dot(cot, up_ref[:, tiles[index + 1]], (1, 0))
        total = (
            dot(cott_ref[:, :half], s0_ref[:, cols], (1, 0))
            + dot(cott_ref[:, half:], s1_ref[:, cols], (1, 0))
            + dot(xt_ref[:, :half], pre0, (1, 0))
            + dot(xt_ref[:, half:], pre1, (1, 0))
        )
        for p in range(parts):
            out_refs[p][:, cols] = total[p * width : (p + 1) * width].astype(out_refs[p].dtype)


def sum_kernel(scale, parts, *refs):
    slice_refs, square_refs, (out_ref, penalty_ref) = refs[:parts], refs[parts:-2], refs[-2:]
    total = slice_refs[0][...]
    for ref in slice_refs[1:]:
        total = total + ref[...].astype(F32)
    out_ref[...] = total.astype(BF16)
    square = square_refs[0][...]
    for ref in square_refs[1:]:
        square = square + ref[...]
    penalty_ref[0, 0] = square[0, 0] * scale


def call(kernel, out_shape, vmem_mib, flops, bytes_accessed, **kwargs):
    return pl.pallas_call(
        kernel,
        out_shape=out_shape,
        compiler_params=pltpu.CompilerParams(vmem_limit_bytes=vmem_mib * MIB),
        cost_estimate=pl.CostEstimate(
            flops=flops, bytes_accessed=bytes_accessed, transcendentals=0
        ),
        **kwargs,
    )


def shift(array, axis, mask):
    size = lax.axis_size(axis)
    return lax.ppermute(array, axis, [(i, i ^ mask) for i in range(size)])


def exchange(blocks):
    if len(blocks) == 1:
        return [lax.all_to_all(blocks[0], "expert", split_axis=0, concat_axis=0, tiled=True)]
    got = {0: blocks[0]}
    for mask in range(1, len(blocks)):
        got[mask] = shift(blocks[mask], "expert", mask)
    return [got[mask] for mask in range(len(blocks))]


def forward(blocks, mask):
    got = []
    for block in blocks:
        got.append(shift(block, "rep", mask))
    return got


def in_vmem(arrays):
    return [pltpu.with_memory_space_constraint(array, pltpu.VMEM) for array in arrays]


def in_hbm(arrays):
    return [pltpu.with_memory_space_constraint(array, pltpu.HBM) for array in arrays]


def body(features, readout, up_weight, down_weight, expert_ids, gate_values):
    tokens, width = features.shape
    hidden = up_weight.shape[2]
    groups, copies = lax.axis_size("expert"), lax.axis_size("rep")
    experts = groups * up_weight.shape[0]
    capacity = (9 * tokens * 2 + 8 * experts - 1) // (8 * experts)
    stride = round_up(capacity + 1, 8)
    slots = experts * stride
    ids = expert_ids.T
    direct = experts <= DIRECT_PEERS
    pieces = experts if direct else 1
    far_mask = copies // 2
    parts = max(1, far_mask)
    part = width // copies
    tile = min(TILE, hidden)

    def blocks_shape(rows):
        if direct:
            return [pltpu.VMEM((rows, width), BF16)] * experts
        return [pltpu.VMEM((experts, rows, width), BF16)]

    rank, *sends = call(
        functools.partial(pack_kernel, experts, capacity),
        [pltpu.VMEM((experts, tokens), jnp.int32)] + blocks_shape(2 * capacity),
        12, 4 * experts * capacity * 2 * tokens * width, 4 * tokens * width * 2,
        in_specs=[ANY] * 3,
        out_specs=[VMEM] * (1 + pieces),
        scratch_shapes=[
            pltpu.VMEM((2, tokens), jnp.int32),
            pltpu.VMEM((2 * tokens, width), BF16),
            pltpu.SemaphoreType.DMA((3,)),
        ],
    )(*in_hbm([ids, features, readout]))
    own = exchange(sends)
    place, flip = call(
        functools.partial(place_kernel, experts, stride),
        [pltpu.VMEM((slots, 2 * tokens), BF16), pltpu.VMEM((2 * tokens, slots), BF16)],
        4, 1 << 20, 1 << 18,
        in_specs=[VMEM, VMEM],
        out_specs=[VMEM] * 2,
    )(ids, *in_vmem([rank]))
    weights = list(call(
        fetch_kernel,
        [pltpu.VMEM((width, hidden), BF16), pltpu.VMEM((hidden, width), BF16)],
        1, 1 << 20, 8 * width * hidden,
        in_specs=[ANY, ANY],
        out_specs=[VMEM] * 2,
        scratch_shapes=[pltpu.SemaphoreType.DMA((2,))],
    )(*in_hbm([up_weight[0], down_weight[0]])))
    far = forward(own, far_mask)

    hidden_shapes = [pltpu.VMEM((slots, hidden), BF16), pltpu.VMEM((slots, hidden), F32)]
    scaled0, pc0, x0, *backs = call(
        functools.partial(own_kernel, experts, capacity, stride, tile, pieces),
        hidden_shapes + [pltpu.VMEM((slots, width), BF16)] + blocks_shape(stride),
        16, 6 * slots * width * hidden, 8 * width * hidden,
        in_specs=[VMEM] * (pieces + 2),
        out_specs=[VMEM] * (pieces + 3),
        scratch_shapes=[pltpu.VMEM((slots, width), BF16)],
    )(*in_vmem(own + weights))
    returned = exchange(backs)
    scaled1, pc1, xt = call(
        functools.partial(far_kernel, experts, capacity, stride, tile, pieces, parts, part),
        hidden_shapes + [pltpu.VMEM((parts * part, 2 * slots), BF16)],
        16, 4 * slots * width * hidden, 8 * width * hidden,
        in_specs=[VMEM] * (pieces + 3),
        out_specs=[VMEM] * 3,
        scratch_shapes=[pltpu.VMEM((slots, width), BF16)] * 2,
    )(*in_vmem(far + [x0] + weights))

    input_grad, *cots = call(
        functools.partial(combine_kernel, experts, capacity, stride, pieces),
        [jax.ShapeDtypeStruct((tokens, width), F32)] + blocks_shape(stride),
        12, 8 * slots * tokens * width, 4 * slots * width + 6 * tokens * width,
        in_specs=[VMEM] * (pieces + 4),
        out_specs=[VMEM] * (1 + pieces),
    )(*in_vmem(returned + [place, flip]), gate_values.T, readout)
    cot_own = exchange(cots)
    cot_far = forward(cot_own, far_mask)

    square, *grads = call(
        functools.partial(grad_kernel, experts, capacity, stride, tile, pieces, parts, part),
        [pltpu.VMEM((8, 128), F32)]
        + [pltpu.VMEM((part, hidden), F32 if p == 0 else BF16) for p in range(parts)],
        20, 4 * slots * width * hidden + 8 * slots * parts * part * hidden,
        2 * width * hidden + 12 * slots * hidden,
        in_specs=[VMEM] * (2 * pieces + 6),
        out_specs=[VMEM] * (1 + parts),
        scratch_shapes=[
            pltpu.VMEM((2 * slots, width), BF16),
            pltpu.VMEM((parts * part, 2 * slots), BF16),
        ],
    )(*in_vmem(cot_own + cot_far + [xt, weights[0], scaled0, scaled1, pc0, pc1]))
    terms = [grads[0]] + [shift(grads[p], "rep", p) for p in range(1, parts)]
    squares = [square] + [shift(square, "rep", p) for p in range(1, parts)]
    grad_up, penalty = call(
        functools.partial(sum_kernel, 1.0 / (2.0 * tokens * groups * copies * width), parts),
        [jax.ShapeDtypeStruct((part, hidden), BF16), jax.ShapeDtypeStruct((1, 1), F32)],
        8, part * hidden, 8 * part * hidden,
        in_specs=[VMEM] * (2 * parts),
        out_specs=[VMEM, SMEM],
    )(*in_vmem(terms + squares))
    return grad_up[None], input_grad, penalty[0, 0]


def solution(mesh):
    both = P(("expert", "rep"), None)
    return jax.shard_map(
        body,
        mesh=mesh,
        in_specs=(both, both, P("expert", None, None), P("expert", None, None), both, both),
        out_specs=(P("expert", "rep", None), both, P()),
        check_vma=False,
    )
```

```python
import functools

import jax
import jax.numpy as jnp
from jax import lax
from jax.experimental import pallas as pl
from jax.experimental.pallas import tpu as pltpu
from jax.sharding import PartitionSpec as P


F32 = jnp.float32
BF16 = jnp.bfloat16
VMEM = pl.BlockSpec(memory_space=pltpu.VMEM)
SMEM = pl.BlockSpec(memory_space=pltpu.SMEM)
ANY = pl.BlockSpec(memory_space=pl.ANY)
MIB = 1 << 20
TILE = 512
GROUPS = ((0, 1, 7, 6), (5, 4, 3, 2))
DIRECT_PEERS = 8


def round_up(value, step):
    return (value + step - 1) // step * step


def dot(left, right, dims):
    return lax.dot_general(left, right, ((dims[:1], dims[1:]), ((), ())), preferred_element_type=F32)


def block_of(refs, index):
    return refs[index] if len(refs) > 1 else refs[0].at[index]


def peers_of(shape):
    block = lax.broadcasted_iota(jnp.int32, shape, 0)
    return block ^ lax.axis_index("expert") if shape[0] <= DIRECT_PEERS else block


def lanes_of(index, width):
    return pl.ds(pl.multiple_of((lax.axis_index("rep") ^ index) * width, width), width)


def pack_kernel(experts, capacity, ids_hbm, x_hbm, r_hbm, rank_ref, *refs):
    *out_refs, ids_ref, rows_ref, sems = refs
    tokens = x_hbm.shape[0]
    copies = [
        pltpu.make_async_copy(ids_hbm, ids_ref, sems.at[0]),
        pltpu.make_async_copy(x_hbm, rows_ref.at[pl.ds(0, tokens)], sems.at[1]),
        pltpu.make_async_copy(r_hbm, rows_ref.at[pl.ds(tokens, tokens)], sems.at[2]),
    ]
    for copy in copies:
        copy.start()
    copies[0].wait()
    peer = peers_of((experts, tokens))
    named = (ids_ref[0:1, :] == peer) | (ids_ref[1:2, :] == peer)
    row = lax.broadcasted_iota(jnp.int32, (tokens, tokens), 0)
    col = lax.broadcasted_iota(jnp.int32, (tokens, tokens), 1)
    before = jnp.where(row < col, 1.0, 0.0).astype(BF16)
    rank = dot(jnp.where(named, 1.0, 0.0).astype(BF16), before, (1, 0))
    rank_x = jnp.where(named, rank, -1.0).astype(jnp.int32)
    rank_r = jnp.where(named, rank + capacity, -1.0).astype(jnp.int32)
    rank_ref[...] = rank_x
    both = jnp.concatenate([rank_x, rank_r], axis=1)
    stride = round_up(2 * capacity, 8)
    slot = lax.broadcasted_iota(jnp.int32, (stride, 2 * tokens), 0)
    placing = jnp.concatenate(
        [jnp.where(slot == both[e : e + 1, :], 1.0, 0.0) for e in range(experts)], axis=0
    ).astype(BF16)
    for copy in copies[1:]:
        copy.wait()
    packed = dot(placing, rows_ref[...], (1, 0))
    for e in range(experts):
        block_of(out_refs, e)[...] = packed[e * stride : e * stride + 2 * capacity].astype(BF16)


def place_kernel(experts, stride, ids_ref, rank_ref, out_ref, flip_ref):
    tokens = ids_ref.shape[1]
    peer = peers_of((experts, tokens))
    rank = rank_ref[...]
    both = jnp.concatenate(
        [jnp.where(ids_ref[k : k + 1, :] == peer, rank, -1) for k in range(2)], axis=1
    )
    slot = lax.broadcasted_iota(jnp.int32, (stride, 2 * tokens), 0)
    placing = jnp.concatenate(
        [jnp.where(slot == both[e : e + 1, :], 1.0, 0.0) for e in range(experts)], axis=0
    )
    out_ref[...] = placing.astype(BF16)
    flip_ref[...] = placing.T.astype(BF16)


def fetch_kernel(up_hbm, down_hbm, up_ref, down_ref, sems):
    copies = [
        pltpu.make_async_copy(up_hbm, up_ref, sems.at[0]),
        pltpu.make_async_copy(down_hbm, down_ref, sems.at[1]),
    ]
    for copy in copies:
        copy.start()
    for copy in copies:
        copy.wait()


def gather_rows(in_refs, order, capacity, stride, x_ref, r_ref):
    pad = jnp.zeros((stride - capacity, x_ref.shape[1]), F32)
    for place, e in enumerate(order):
        block = block_of(in_refs, e)[...].astype(F32)
        where = pl.ds(place * stride, stride)
        x_ref[where, :] = jnp.concatenate([block[:capacity], pad], axis=0).astype(BF16)
        r_ref[where, :] = jnp.concatenate([block[capacity:], pad], axis=0).astype(BF16)


def hidden_of(x, r, up_ref, down_ref, cols, scaled_ref, pc_ref):
    pre = dot(x, up_ref[:, cols], (1, 0))
    proj = dot(r, down_ref[cols, :], (1, 1))
    gate = 1.0 / (1.0 + jnp.exp(-pre))
    rest = 1.0 - gate
    slope = gate * (1.0 + pre * rest)
    curve = gate * rest * (2.0 + pre * (1.0 - 2.0 * gate))
    scaled = (slope * proj).astype(BF16)
    scaled_ref[:, cols] = scaled
    pc_ref[:, cols] = proj * curve
    return scaled


def tiles_of(hidden, tile):
    return [slice(at, at + tile) for at in range(0, hidden, tile)]


def own_kernel(experts, capacity, stride, tile, n_in, *refs):
    in_refs, (up_ref, down_ref), refs = refs[:n_in], refs[n_in : n_in + 2], refs[n_in + 2 :]
    scaled_ref, pc_ref, x_ref, *back_refs, r_ref = refs
    gather_rows(in_refs, range(experts), capacity, stride, x_ref, r_ref)
    x, r = x_ref[...], r_ref[...]
    back, late = None, None
    for cols in tiles_of(up_ref.shape[1], tile):
        scaled = hidden_of(x, r, up_ref, down_ref, cols, scaled_ref, pc_ref)
        if late is not None:
            term = dot(late[0], up_ref[:, late[1]], (1, 1))
            back = term if back is None else back + term
        late = scaled, cols
    term = dot(late[0], up_ref[:, late[1]], (1, 1))
    back = term if back is None else back + term
    for e in range(experts):
        block_of(back_refs, e)[...] = back[e * stride : (e + 1) * stride].astype(BF16)


def far_kernel(order, capacity, stride, tile, n_in, parts, width, *refs):
    in_refs, refs = refs[:n_in], refs[n_in:]
    *own_refs, up_ref, down_ref, scaled_ref, pc_ref, own_t_ref, far_t_ref, x_ref, r_ref = refs
    gather_rows(in_refs, order, capacity, stride, x_ref, r_ref)
    x, r = x_ref[...], r_ref[...]
    for cols in tiles_of(up_ref.shape[1], tile):
        hidden_of(x, r, up_ref, down_ref, cols, scaled_ref, pc_ref)
    for p in range(parts):
        lanes, into = lanes_of(p, width), slice(p * width, (p + 1) * width)
        own_t_ref[into, :] = jnp.concatenate([ref[:, lanes] for ref in own_refs], axis=0).T
        far_t_ref[into, :] = x_ref[:, lanes].T


def combine_kernel(experts, capacity, stride, n_in, *refs):
    in_refs, refs = refs[:n_in], refs[n_in:]
    place_ref, flip_ref, gate_ref, r_ref, grad_ref, *out_refs = refs
    tokens = r_ref.shape[0]
    rows = jnp.concatenate(
        [block_of(in_refs, e)[...].astype(F32) for e in range(experts)], axis=0
    ).astype(BF16)
    pairs = dot(flip_ref[...], rows, (1, 0))
    gates = jnp.concatenate([gate_ref[...], jnp.zeros((6, tokens), F32)], axis=0).T
    gate0, gate1 = gates[:, 0:1], gates[:, 1:2]
    grad = r_ref[...].astype(F32) + gate0 * pairs[:tokens] + gate1 * pairs[tokens:]
    grad_ref[...] = grad
    cot = jnp.concatenate([(gate0 * grad).astype(BF16), (gate1 * grad).astype(BF16)], axis=0)
    sent = dot(place_ref[...], cot, (1, 0))
    square = jnp.full((stride, r_ref.shape[1]), jnp.sum(grad * grad), F32)
    high = square.astype(BF16).astype(F32)
    middle = (square - high).astype(BF16).astype(F32)
    lane = lax.broadcasted_iota(jnp.int32, square.shape, 1)
    row = lax.broadcasted_iota(jnp.int32, square.shape, 0)
    terms = jnp.where(lane < 128, high, jnp.where(lane < 256, middle, square - high - middle))
    for e in range(experts):
        block = jnp.where(row == capacity, terms, sent[e * stride : (e + 1) * stride])
        block_of(out_refs, e)[...] = block.astype(BF16)


def square_of(blocks, capacity):
    low = capacity // 8 * 8
    sums = []
    for block in blocks:
        row = block[low : low + 8, :384].astype(F32)[capacity - low : capacity - low + 1]
        sums.append(row[:, :128] + row[:, 128:256] + row[:, 256:])
    while len(sums) > 1:
        sums = [sums[i] + sums[i + 1] for i in range(0, len(sums), 2)]
    return sums[0]


def gather_cots(in_refs, order, capacity, stride, parts, width, xt_ref, cot_ref, rows_ref):
    blocks = [block_of(in_refs, e)[...] for e in range(len(order))]
    for place, e in enumerate(order):
        cot_ref[place * stride : (place + 1) * stride, :] = blocks[e]
    slots = cot_ref.shape[0]
    for p in range(parts):
        rows_ref[p * width : (p + 1) * width, :slots] = cot_ref[:, lanes_of(p, width)].T
    rows_ref[:, slots:] = xt_ref[...]
    return square_of(blocks, capacity)


def read_cols(refs, cols):
    return jnp.concatenate([ref[:, cols] for ref in refs], axis=0)


def grad_own_kernel(order, capacity, stride, tile, n_in, groups, parts, width, *refs):
    in_refs, refs = refs[:n_in], refs[n_in:]
    scaled_refs, pc_refs, refs = refs[:groups], refs[groups : 2 * groups], refs[2 * groups :]
    xt_ref, up_ref, square_ref, acc_ref, cot_ref, rows_ref = refs
    square = gather_cots(
        in_refs, order, capacity, stride, parts, width, xt_ref, cot_ref, rows_ref
    )
    square_ref[...] = jnp.broadcast_to(square, square_ref.shape)
    cot, rows = cot_ref[...], rows_ref[...]
    tiles = tiles_of(up_ref.shape[1], tile)
    slope_grad = dot(cot, up_ref[:, tiles[0]], (1, 0))
    for index, cols in enumerate(tiles):
        pre_grad = (slope_grad * read_cols(pc_refs, cols)).astype(BF16)
        if index + 1 < len(tiles):
            slope_grad = dot(cot, up_ref[:, tiles[index + 1]], (1, 0))
        terms = jnp.concatenate([ref[:, cols] for ref in scaled_refs] + [pre_grad], axis=0)
        acc_ref[:, cols] = dot(rows, terms, (1, 0))


def grad_far_kernel(order, capacity, stride, tile, n_in, parts, width, *refs):
    in_refs, refs = refs[:n_in], refs[n_in:]
    xt_ref, up_ref, scaled_ref, pc_ref, acc_ref, part_ref, *refs = refs
    square_ref, pre_grad_ref, rows_ref, *out_refs, cot_ref = refs
    square = gather_cots(
        in_refs, order, capacity, stride, parts, width, xt_ref, cot_ref, rows_ref
    )
    square_ref[...] = part_ref[...] + jnp.broadcast_to(square, square_ref.shape)
    cot, rows = cot_ref[...], rows_ref[width:, :]
    tiles = tiles_of(up_ref.shape[1], tile)
    slope_grad = dot(cot, up_ref[:, tiles[0]], (1, 0))
    for index, cols in enumerate(tiles):
        pre_grad = (slope_grad * pc_ref[:, cols]).astype(BF16)
        pre_grad_ref[:, cols] = pre_grad
        if index + 1 < len(tiles):
            slope_grad = dot(cot, up_ref[:, tiles[index + 1]], (1, 0))
        if parts > 1:
            terms = jnp.concatenate([scaled_ref[:, cols], pre_grad], axis=0)
            total = acc_ref[width:, cols] + dot(rows, terms, (1, 0))
            for p in range(1, parts):
                out_refs[p - 1][:, cols] = total[(p - 1) * width : p * width].astype(BF16)


def grad_keep_kernel(width, tile, rows_ref, scaled_ref, pre_grad_ref, acc_ref, out_ref):
    rows = rows_ref[:width, :]
    for cols in tiles_of(acc_ref.shape[1], tile):
        terms = read_cols([scaled_ref, pre_grad_ref], cols)
        out_ref[:, cols] = acc_ref[:width, cols] + dot(rows, terms, (1, 0))


def sum_kernel(scale, parts, *refs):
    slice_refs, square_refs, (out_ref, penalty_ref) = refs[:parts], refs[parts:-2], refs[-2:]
    total = slice_refs[0][...]
    for ref in slice_refs[1:]:
        total = total + ref[...].astype(F32)
    out_ref[...] = total.astype(BF16)
    square = square_refs[0][...]
    for ref in square_refs[1:]:
        square = square + ref[...]
    penalty_ref[0, 0] = square[0, 0] * scale


def call(kernel, out_shape, vmem_mib, flops, bytes_accessed, **kwargs):
    return pl.pallas_call(
        kernel,
        out_shape=out_shape,
        compiler_params=pltpu.CompilerParams(vmem_limit_bytes=vmem_mib * MIB),
        cost_estimate=pl.CostEstimate(
            flops=flops, bytes_accessed=bytes_accessed, transcendentals=0
        ),
        **kwargs,
    )


def shift(array, axis, mask):
    size = lax.axis_size(axis)
    return lax.ppermute(array, axis, [(i, i ^ mask) for i in range(size)])


def exchange(blocks):
    if len(blocks) == 1:
        return [lax.all_to_all(blocks[0], "expert", split_axis=0, concat_axis=0, tiled=True)]
    got = {0: blocks[0]}
    for mask in range(1, len(blocks)):
        got[mask] = shift(blocks[mask], "expert", mask)
    return [got[mask] for mask in range(len(blocks))]


def forward(blocks, mask):
    got = []
    for block in blocks:
        got.append(shift(block, "rep", mask))
    return got


def in_vmem(arrays):
    return [pltpu.with_memory_space_constraint(array, pltpu.VMEM) for array in arrays]


def in_hbm(arrays):
    return [pltpu.with_memory_space_constraint(array, pltpu.HBM) for array in arrays]


def body(features, readout, up_weight, down_weight, expert_ids, gate_values):
    tokens, width = features.shape
    hidden = up_weight.shape[2]
    groups, copies = lax.axis_size("expert"), lax.axis_size("rep")
    experts = groups * up_weight.shape[0]
    capacity = (9 * tokens * 2 + 8 * experts - 1) // (8 * experts)
    stride = round_up(capacity + 1, 8)
    slots = experts * stride
    ids = expert_ids.T
    direct = experts <= DIRECT_PEERS
    pieces = experts if direct else 1
    far_mask = copies // 2
    parts = max(1, far_mask)
    part = width // copies
    tile = min(TILE, hidden)

    def blocks_shape(rows):
        if direct:
            return [pltpu.VMEM((rows, width), BF16)] * experts
        return [pltpu.VMEM((experts, rows, width), BF16)]

    rank, *sends = call(
        functools.partial(pack_kernel, experts, capacity),
        [pltpu.VMEM((experts, tokens), jnp.int32)] + blocks_shape(2 * capacity),
        12, 4 * experts * capacity * 2 * tokens * width, 4 * tokens * width * 2,
        in_specs=[ANY] * 3,
        out_specs=[VMEM] * (1 + pieces),
        scratch_shapes=[
            pltpu.VMEM((2, tokens), jnp.int32),
            pltpu.VMEM((2 * tokens, width), BF16),
            pltpu.SemaphoreType.DMA((3,)),
        ],
    )(*in_hbm([ids, features, readout]))
    own = exchange(sends)
    place, flip = call(
        functools.partial(place_kernel, experts, stride),
        [pltpu.VMEM((slots, 2 * tokens), BF16), pltpu.VMEM((2 * tokens, slots), BF16)],
        4, 1 << 20, 1 << 18,
        in_specs=[VMEM, VMEM],
        out_specs=[VMEM] * 2,
    )(ids, *in_vmem([rank]))
    weights = list(call(
        fetch_kernel,
        [pltpu.VMEM((width, hidden), BF16), pltpu.VMEM((hidden, width), BF16)],
        1, 1 << 20, 8 * width * hidden,
        in_specs=[ANY, ANY],
        out_specs=[VMEM] * 2,
        scratch_shapes=[pltpu.SemaphoreType.DMA((2,))],
    )(*in_hbm([up_weight[0], down_weight[0]])))
    far = forward(own, far_mask)

    groups_of = GROUPS if direct and experts == DIRECT_PEERS else (tuple(range(pieces)),)
    order = sum(groups_of, ()) if direct else tuple(range(experts))
    scaled0, pc0, x0, backs = [], [], [], [None] * pieces
    for group in groups_of:
        count = len(group) if direct else experts
        rows = count * stride
        scaled, pc, x, *sent = call(
            functools.partial(own_kernel, count, capacity, stride, tile, len(group)),
            [
                pltpu.VMEM((rows, hidden), BF16),
                pltpu.VMEM((rows, hidden), F32),
                pltpu.VMEM((rows, width), BF16),
            ]
            + blocks_shape(stride)[: len(group)],
            16, 6 * rows * width * hidden, 8 * width * hidden,
            in_specs=[VMEM] * (len(group) + 2),
            out_specs=[VMEM] * (len(group) + 3),
            scratch_shapes=[pltpu.VMEM((rows, width), BF16)],
        )(*in_vmem([own[e] for e in group] + weights))
        scaled0.append(scaled)
        pc0.append(pc)
        x0.append(x)
        for e, block in zip(group, sent):
            backs[e] = block
    returned = exchange(backs)
    rows_t = pltpu.VMEM((parts * part, slots), BF16)
    scaled1, pc1, own_t, far_t = call(
        functools.partial(far_kernel, order, capacity, stride, tile, pieces, parts, part),
        [pltpu.VMEM((slots, hidden), BF16), pltpu.VMEM((slots, hidden), F32), rows_t, rows_t],
        16, 4 * slots * width * hidden, 8 * width * hidden,
        in_specs=[VMEM] * (pieces + len(x0) + 2),
        out_specs=[VMEM] * 4,
        scratch_shapes=[pltpu.VMEM((slots, width), BF16)] * 2,
    )(*in_vmem(far + x0 + weights))

    input_grad, *cots = call(
        functools.partial(combine_kernel, experts, capacity, stride, pieces),
        [jax.ShapeDtypeStruct((tokens, width), F32)] + blocks_shape(stride),
        12, 8 * slots * tokens * width, 4 * slots * width + 6 * tokens * width,
        in_specs=[VMEM] * (pieces + 4),
        out_specs=[VMEM] * (1 + pieces),
    )(*in_vmem(returned + [place, flip]), gate_values.T, readout)
    cot_own = exchange(cots)
    cot_far = forward(cot_own, far_mask)

    flops = 2 * slots * width * hidden + 4 * slots * parts * part * hidden
    both_t = pltpu.VMEM((parts * part, 2 * slots), BF16)
    square, acc = call(
        functools.partial(
            grad_own_kernel, order, capacity, stride, tile, pieces, len(x0), parts, part
        ),
        [pltpu.VMEM((8, 128), F32), pltpu.VMEM((parts * part, hidden), F32)],
        16, flops, 2 * width * hidden,
        in_specs=[VMEM] * (pieces + 2 * len(x0) + 2),
        out_specs=[VMEM] * 2,
        scratch_shapes=[pltpu.VMEM((slots, width), BF16), both_t],
    )(*in_vmem(cot_own + scaled0 + pc0 + [own_t, weights[0]]))
    square, pre_grad, far_rows, *sent = call(
        functools.partial(grad_far_kernel, order, capacity, stride, tile, pieces, parts, part),
        [pltpu.VMEM((8, 128), F32), pltpu.VMEM((slots, hidden), BF16), both_t]
        + [pltpu.VMEM((part, hidden), BF16)] * (parts - 1),
        16, flops, 2 * width * hidden,
        in_specs=[VMEM] * (pieces + 6),
        out_specs=[VMEM] * (2 + parts),
        scratch_shapes=[pltpu.VMEM((slots, width), BF16)],
    )(*in_vmem(cot_far + [far_t, weights[0], scaled1, pc1, acc, square]))
    kept = call(
        functools.partial(grad_keep_kernel, part, tile),
        pltpu.VMEM((part, hidden), F32),
        12, 4 * slots * part * hidden, 2 * part * hidden,
        in_specs=[VMEM] * 4,
        out_specs=VMEM,
    )(*in_vmem([far_rows, scaled1, pre_grad, acc]))
    came = [shift(sent[p - 1], "rep", p) for p in range(1, parts)]
    terms = [kept] + came
    squares = [square] + [shift(square, "rep", p) for p in range(1, parts)]
    grad_up, penalty = call(
        functools.partial(sum_kernel, 1.0 / (2.0 * tokens * groups * copies * width), parts),
        [jax.ShapeDtypeStruct((part, hidden), BF16), jax.ShapeDtypeStruct((1, 1), F32)],
        8, part * hidden, 8 * part * hidden,
        in_specs=[VMEM] * (2 * parts),
        out_specs=[VMEM, SMEM],
    )(*in_vmem(terms + squares))
    return grad_up[None], input_grad, penalty[0, 0]


def solution(mesh):
    both = P(("expert", "rep"), None)
    return jax.shard_map(
        body,
        mesh=mesh,
        in_specs=(both, both, P("expert", None, None), P("expert", None, None), both, both),
        out_specs=(P("expert", "rep", None), both, P()),
        check_vma=False,
    )
```

```python
import functools

import jax
import jax.numpy as jnp
from jax import lax
from jax.experimental import pallas as pl
from jax.experimental.pallas import tpu as pltpu
from jax.sharding import PartitionSpec as P


F32 = jnp.float32
BF16 = jnp.bfloat16
VMEM = pl.BlockSpec(memory_space=pltpu.VMEM)
SMEM = pl.BlockSpec(memory_space=pltpu.SMEM)
ANY = pl.BlockSpec(memory_space=pl.ANY)
MIB = 1 << 20
TILE = 512
GROUPS = ((0, 1, 7, 6), (5, 4, 3, 2))
PAIRS = ((0, 1), (7, 6), (3, 2), (5, 4))
DIRECT_PEERS = 8


def round_up(value, step):
    return (value + step - 1) // step * step


def dot(left, right, dims):
    return lax.dot_general(left, right, ((dims[:1], dims[1:]), ((), ())), preferred_element_type=F32)


def block_of(refs, index):
    return refs[index] if len(refs) > 1 else refs[0].at[index]


def peers_of(shape):
    block = lax.broadcasted_iota(jnp.int32, shape, 0)
    return block ^ lax.axis_index("expert") if shape[0] <= DIRECT_PEERS else block


def lanes_of(index, width):
    return pl.ds(pl.multiple_of((lax.axis_index("rep") ^ index) * width, width), width)


def pack_kernel(experts, capacity, ids_hbm, x_hbm, r_hbm, rank_ref, *refs):
    *out_refs, ids_ref, rows_ref, sems = refs
    tokens = x_hbm.shape[0]
    copies = [
        pltpu.make_async_copy(ids_hbm, ids_ref, sems.at[0]),
        pltpu.make_async_copy(x_hbm, rows_ref.at[pl.ds(0, tokens)], sems.at[1]),
        pltpu.make_async_copy(r_hbm, rows_ref.at[pl.ds(tokens, tokens)], sems.at[2]),
    ]
    for copy in copies:
        copy.start()
    copies[0].wait()
    peer = peers_of((experts, tokens))
    named = (ids_ref[0:1, :] == peer) | (ids_ref[1:2, :] == peer)
    row = lax.broadcasted_iota(jnp.int32, (tokens, tokens), 0)
    col = lax.broadcasted_iota(jnp.int32, (tokens, tokens), 1)
    before = jnp.where(row < col, 1.0, 0.0).astype(BF16)
    rank = dot(jnp.where(named, 1.0, 0.0).astype(BF16), before, (1, 0))
    rank_x = jnp.where(named, rank, -1.0).astype(jnp.int32)
    rank_r = jnp.where(named, rank + capacity, -1.0).astype(jnp.int32)
    rank_ref[...] = rank_x
    both = jnp.concatenate([rank_x, rank_r], axis=1)
    stride = round_up(2 * capacity, 8)
    slot = lax.broadcasted_iota(jnp.int32, (stride, 2 * tokens), 0)
    placing = jnp.concatenate(
        [jnp.where(slot == both[e : e + 1, :], 1.0, 0.0) for e in range(experts)], axis=0
    ).astype(BF16)
    for copy in copies[1:]:
        copy.wait()
    packed = dot(placing, rows_ref[...], (1, 0))
    for e in range(experts):
        block_of(out_refs, e)[...] = packed[e * stride : e * stride + 2 * capacity].astype(BF16)


def place_kernel(experts, stride, ids_ref, rank_ref, out_ref, flip_ref):
    tokens = ids_ref.shape[1]
    peer = peers_of((experts, tokens))
    rank = rank_ref[...]
    both = jnp.concatenate(
        [jnp.where(ids_ref[k : k + 1, :] == peer, rank, -1) for k in range(2)], axis=1
    )
    slot = lax.broadcasted_iota(jnp.int32, (stride, 2 * tokens), 0)
    placing = jnp.concatenate(
        [jnp.where(slot == both[e : e + 1, :], 1.0, 0.0) for e in range(experts)], axis=0
    )
    out_ref[...] = placing.astype(BF16)
    flip_ref[...] = placing.T.astype(BF16)


def fetch_kernel(up_hbm, down_hbm, up_ref, down_ref, sems):
    copies = [
        pltpu.make_async_copy(up_hbm, up_ref, sems.at[0]),
        pltpu.make_async_copy(down_hbm, down_ref, sems.at[1]),
    ]
    for copy in copies:
        copy.start()
    for copy in copies:
        copy.wait()


def gather_rows(in_refs, order, capacity, stride, x_ref, r_ref):
    pad = jnp.zeros((stride - capacity, x_ref.shape[1]), F32)
    for place, e in enumerate(order):
        block = block_of(in_refs, e)[...].astype(F32)
        where = pl.ds(place * stride, stride)
        x_ref[where, :] = jnp.concatenate([block[:capacity], pad], axis=0).astype(BF16)
        r_ref[where, :] = jnp.concatenate([block[capacity:], pad], axis=0).astype(BF16)


def hidden_of(x, r, up_ref, down_ref, cols, scaled_ref, pc_ref):
    pre = dot(x, up_ref[:, cols], (1, 0))
    proj = dot(r, down_ref[cols, :], (1, 1))
    gate = 1.0 / (1.0 + jnp.exp(-pre))
    rest = 1.0 - gate
    slope = gate * (1.0 + pre * rest)
    curve = gate * rest * (2.0 + pre * (1.0 - 2.0 * gate))
    scaled = (slope * proj).astype(BF16)
    scaled_ref[:, cols] = scaled
    pc_ref[:, cols] = proj * curve
    return scaled


def tiles_of(hidden, tile):
    return [slice(at, at + tile) for at in range(0, hidden, tile)]


def own_kernel(experts, capacity, stride, tile, n_in, *refs):
    in_refs, (up_ref, down_ref), refs = refs[:n_in], refs[n_in : n_in + 2], refs[n_in + 2 :]
    scaled_ref, pc_ref, x_ref, *back_refs, r_ref = refs
    gather_rows(in_refs, range(experts), capacity, stride, x_ref, r_ref)
    x, r = x_ref[...], r_ref[...]
    back, late = None, None
    for cols in tiles_of(up_ref.shape[1], tile):
        scaled = hidden_of(x, r, up_ref, down_ref, cols, scaled_ref, pc_ref)
        if late is not None:
            term = dot(late[0], up_ref[:, late[1]], (1, 1))
            back = term if back is None else back + term
        late = scaled, cols
    term = dot(late[0], up_ref[:, late[1]], (1, 1))
    back = term if back is None else back + term
    for e in range(experts):
        block_of(back_refs, e)[...] = back[e * stride : (e + 1) * stride].astype(BF16)


def far_kernel(order, capacity, stride, tile, n_in, parts, width, *refs):
    in_refs, refs = refs[:n_in], refs[n_in:]
    *own_refs, up_ref, down_ref, scaled_ref, pc_ref, own_t_ref, far_t_ref, x_ref, r_ref = refs
    gather_rows(in_refs, order, capacity, stride, x_ref, r_ref)
    x, r = x_ref[...], r_ref[...]
    for cols in tiles_of(up_ref.shape[1], tile):
        hidden_of(x, r, up_ref, down_ref, cols, scaled_ref, pc_ref)
    for p in range(parts):
        lanes, into = lanes_of(p, width), slice(p * width, (p + 1) * width)
        own_t_ref[into, :] = jnp.concatenate([ref[:, lanes] for ref in own_refs], axis=0).T
        far_t_ref[into, :] = x_ref[:, lanes].T


def combine_kernel(experts, capacity, stride, n_in, *refs):
    in_refs, refs = refs[:n_in], refs[n_in:]
    place_ref, flip_ref, gate_ref, r_ref, grad_ref, *out_refs = refs
    tokens = r_ref.shape[0]
    rows = jnp.concatenate(
        [block_of(in_refs, e)[...].astype(F32) for e in range(experts)], axis=0
    ).astype(BF16)
    pairs = dot(flip_ref[...], rows, (1, 0))
    gates = jnp.concatenate([gate_ref[...], jnp.zeros((6, tokens), F32)], axis=0).T
    gate0, gate1 = gates[:, 0:1], gates[:, 1:2]
    grad = r_ref[...].astype(F32) + gate0 * pairs[:tokens] + gate1 * pairs[tokens:]
    grad_ref[...] = grad
    cot = jnp.concatenate([(gate0 * grad).astype(BF16), (gate1 * grad).astype(BF16)], axis=0)
    sent = dot(place_ref[...], cot, (1, 0))
    square = jnp.full((stride, r_ref.shape[1]), jnp.sum(grad * grad), F32)
    high = square.astype(BF16).astype(F32)
    middle = (square - high).astype(BF16).astype(F32)
    lane = lax.broadcasted_iota(jnp.int32, square.shape, 1)
    row = lax.broadcasted_iota(jnp.int32, square.shape, 0)
    terms = jnp.where(lane < 128, high, jnp.where(lane < 256, middle, square - high - middle))
    for e in range(experts):
        block = jnp.where(row == capacity, terms, sent[e * stride : (e + 1) * stride])
        block_of(out_refs, e)[...] = block.astype(BF16)


def square_of(blocks, capacity):
    low = capacity // 8 * 8
    sums = []
    for block in blocks:
        row = block[low : low + 8, :384].astype(F32)[capacity - low : capacity - low + 1]
        sums.append(row[:, :128] + row[:, 128:256] + row[:, 256:])
    while len(sums) > 1:
        sums = [sums[i] + sums[i + 1] for i in range(0, len(sums), 2)]
    return sums[0]


def join_kernel(capacity, *refs):
    rows = [ref[...].astype(F32)[:capacity] for ref in refs[:-1]]
    refs[-1][...] = jnp.concatenate(rows, axis=0).astype(BF16)


def transpose_rows(parts, width, xt_ref, cot_ref, rows_ref):
    slots = cot_ref.shape[0]
    for p in range(parts):
        rows_ref[p * width : (p + 1) * width, :slots] = cot_ref[:, lanes_of(p, width)].T
    rows_ref[:, slots:] = xt_ref[...]


def read_cols(refs, cols):
    return jnp.concatenate([ref[:, cols] for ref in refs], axis=0)


def grad_own_kernel(order, capacity, stride, tile, n_in, groups, parts, width, *refs):
    in_refs, refs = refs[:n_in], refs[n_in:]
    scaled_refs, pc_refs, refs = refs[:groups], refs[groups : 2 * groups], refs[2 * groups :]
    xt_ref, up_ref, grad_ref, square_ref, acc_ref, grad_hbm, cot_ref, rows_ref, sem = refs
    copy = pltpu.make_async_copy(grad_ref, grad_hbm, sem)
    copy.start()
    blocks = [None] * len(order)
    for place, e in enumerate(order):
        blocks[e] = block_of(in_refs, place)[...]
        cot_ref[place * stride : (place + 1) * stride, :] = blocks[e]
    square_ref[...] = jnp.broadcast_to(square_of(blocks, capacity), square_ref.shape)
    transpose_rows(parts, width, xt_ref, cot_ref, rows_ref)
    cot, rows = cot_ref[...], rows_ref[...]
    tiles = tiles_of(up_ref.shape[1], tile)
    slope_grad = dot(cot, up_ref[:, tiles[0]], (1, 0))
    for index, cols in enumerate(tiles):
        pre_grad = (slope_grad * read_cols(pc_refs, cols)).astype(BF16)
        if index + 1 < len(tiles):
            slope_grad = dot(cot, up_ref[:, tiles[index + 1]], (1, 0))
        terms = jnp.concatenate([ref[:, cols] for ref in scaled_refs] + [pre_grad], axis=0)
        acc_ref[:, cols] = dot(rows, terms, (1, 0))
    copy.wait()


def grad_far_kernel(experts, capacity, stride, tile, n_in, parts, width, *refs):
    in_refs, refs = refs[:n_in], refs[n_in:]
    xt_ref, up_ref, scaled_ref, pc_ref, acc_ref, *refs = refs
    pre_grad_ref, rows_ref, *out_refs, cot_ref = refs
    pad = jnp.zeros((stride - capacity, cot_ref.shape[1]), F32)
    share = experts // n_in
    for place in range(experts):
        ref, at = in_refs[place // share], place % share
        if len(ref.shape) == 3:
            block = ref[at].astype(F32)[:capacity]
        else:
            block = ref[...].astype(F32)[at * capacity : (at + 1) * capacity]
        into = slice(place * stride, (place + 1) * stride)
        cot_ref[into, :] = jnp.concatenate([block, pad], axis=0).astype(BF16)
    transpose_rows(parts, width, xt_ref, cot_ref, rows_ref)
    cot, rows = cot_ref[...], rows_ref[width:, :]
    tiles = tiles_of(up_ref.shape[1], tile)
    slope_grad = dot(cot, up_ref[:, tiles[0]], (1, 0))
    for index, cols in enumerate(tiles):
        pre_grad = (slope_grad * pc_ref[:, cols]).astype(BF16)
        pre_grad_ref[:, cols] = pre_grad
        if index + 1 < len(tiles):
            slope_grad = dot(cot, up_ref[:, tiles[index + 1]], (1, 0))
        if parts > 1:
            terms = jnp.concatenate([scaled_ref[:, cols], pre_grad], axis=0)
            total = acc_ref[width:, cols] + dot(rows, terms, (1, 0))
            for p in range(1, parts):
                out_refs[p - 1][:, cols] = total[(p - 1) * width : p * width].astype(BF16)


def grad_keep_kernel(width, tile, *refs):
    rows_ref, scaled_ref, pre_grad_ref, acc_ref, own_ref, far_ref, out_ref, square_ref = refs
    square_ref[...] = own_ref[...] + far_ref[...]
    rows = rows_ref[:width, :]
    for cols in tiles_of(acc_ref.shape[1], tile):
        terms = read_cols([scaled_ref, pre_grad_ref], cols)
        out_ref[:, cols] = acc_ref[:width, cols] + dot(rows, terms, (1, 0))


def sum_kernel(scale, parts, *refs):
    slice_refs, square_refs, (out_ref, penalty_ref) = refs[:parts], refs[parts:-2], refs[-2:]
    total = slice_refs[0][...]
    for ref in slice_refs[1:]:
        total = total + ref[...].astype(F32)
    out_ref[...] = total.astype(BF16)
    square = square_refs[0][...]
    for ref in square_refs[1:]:
        square = square + ref[...]
    penalty_ref[0, 0] = square[0, 0] * scale


def call(kernel, out_shape, vmem_mib, flops, bytes_accessed, **kwargs):
    return pl.pallas_call(
        kernel,
        out_shape=out_shape,
        compiler_params=pltpu.CompilerParams(vmem_limit_bytes=vmem_mib * MIB),
        cost_estimate=pl.CostEstimate(
            flops=flops, bytes_accessed=bytes_accessed, transcendentals=0
        ),
        **kwargs,
    )


def shift(array, axis, mask):
    size = lax.axis_size(axis)
    return lax.ppermute(array, axis, [(i, i ^ mask) for i in range(size)])


def exchange(blocks):
    if len(blocks) == 1:
        return [lax.all_to_all(blocks[0], "expert", split_axis=0, concat_axis=0, tiled=True)]
    got = {0: blocks[0]}
    for mask in range(1, len(blocks)):
        got[mask] = shift(blocks[mask], "expert", mask)
    return [got[mask] for mask in range(len(blocks))]


def forward(blocks, mask):
    got = []
    for block in blocks:
        got.append(shift(block, "rep", mask))
    return got


def in_vmem(arrays):
    return [pltpu.with_memory_space_constraint(array, pltpu.VMEM) for array in arrays]


def in_order(blocks, order):
    return [blocks[e] for e in order] if len(blocks) > 1 else blocks


def in_hbm(arrays):
    return [pltpu.with_memory_space_constraint(array, pltpu.HBM) for array in arrays]


def body(features, readout, up_weight, down_weight, expert_ids, gate_values):
    tokens, width = features.shape
    hidden = up_weight.shape[2]
    groups, copies = lax.axis_size("expert"), lax.axis_size("rep")
    experts = groups * up_weight.shape[0]
    capacity = (9 * tokens * 2 + 8 * experts - 1) // (8 * experts)
    stride = round_up(capacity + 1, 8)
    slots = experts * stride
    ids = expert_ids.T
    direct = experts <= DIRECT_PEERS
    pieces = experts if direct else 1
    far_mask = copies // 2
    parts = max(1, far_mask)
    part = width // copies
    tile = min(TILE, hidden)

    def blocks_shape(rows):
        if direct:
            return [pltpu.VMEM((rows, width), BF16)] * experts
        return [pltpu.VMEM((experts, rows, width), BF16)]

    rank, *sends = call(
        functools.partial(pack_kernel, experts, capacity),
        [pltpu.VMEM((experts, tokens), jnp.int32)] + blocks_shape(2 * capacity),
        12, 4 * experts * capacity * 2 * tokens * width, 4 * tokens * width * 2,
        in_specs=[ANY] * 3,
        out_specs=[VMEM] * (1 + pieces),
        scratch_shapes=[
            pltpu.VMEM((2, tokens), jnp.int32),
            pltpu.VMEM((2 * tokens, width), BF16),
            pltpu.SemaphoreType.DMA((3,)),
        ],
    )(*in_hbm([ids, features, readout]))
    own = exchange(sends)
    place, flip = call(
        functools.partial(place_kernel, experts, stride),
        [pltpu.VMEM((slots, 2 * tokens), BF16), pltpu.VMEM((2 * tokens, slots), BF16)],
        4, 1 << 20, 1 << 18,
        in_specs=[VMEM, VMEM],
        out_specs=[VMEM] * 2,
    )(ids, *in_vmem([rank]))
    weights = list(call(
        fetch_kernel,
        [pltpu.VMEM((width, hidden), BF16), pltpu.VMEM((hidden, width), BF16)],
        1, 1 << 20, 8 * width * hidden,
        in_specs=[ANY, ANY],
        out_specs=[VMEM] * 2,
        scratch_shapes=[pltpu.SemaphoreType.DMA((2,))],
    )(*in_hbm([up_weight[0], down_weight[0]])))
    far = forward(own, far_mask)

    grouped = experts == DIRECT_PEERS
    groups_of = GROUPS if grouped else (tuple(range(pieces)),)
    pairs_of = PAIRS if grouped else None
    order = sum(groups_of, ()) if direct else tuple(range(experts))
    far_order = sum(pairs_of, ()) if grouped else order
    scaled0, pc0, x0, backs = [], [], [], [None] * pieces
    for group in groups_of:
        count = len(group) if direct else experts
        rows = count * stride
        scaled, pc, x, *sent = call(
            functools.partial(own_kernel, count, capacity, stride, tile // 2, len(group)),
            [
                pltpu.VMEM((rows, hidden), BF16),
                pltpu.VMEM((rows, hidden), F32),
                pltpu.VMEM((rows, width), BF16),
            ]
            + blocks_shape(stride)[: len(group)],
            16, 6 * rows * width * hidden, 8 * width * hidden,
            in_specs=[VMEM] * (len(group) + 2),
            out_specs=[VMEM] * (len(group) + 3),
            scratch_shapes=[pltpu.VMEM((rows, width), BF16)],
        )(*in_vmem([own[e] for e in group] + weights))
        scaled0.append(scaled)
        pc0.append(pc)
        x0.append(x)
        for e, block in zip(group, sent):
            backs[e] = block
    returned = exchange(backs)
    rows_t = pltpu.VMEM((parts * part, slots), BF16)
    scaled1, pc1, own_t, far_t = call(
        functools.partial(far_kernel, far_order, capacity, stride, tile, pieces, parts, part),
        [pltpu.VMEM((slots, hidden), BF16), pltpu.VMEM((slots, hidden), F32), rows_t, rows_t],
        16, 4 * slots * width * hidden, 8 * width * hidden,
        in_specs=[VMEM] * (pieces + len(x0) + 2),
        out_specs=[VMEM] * 4,
        scratch_shapes=[pltpu.VMEM((slots, width), BF16)] * 2,
    )(*in_vmem(far + x0 + weights))

    input_grad, *cots = call(
        functools.partial(combine_kernel, experts, capacity, stride, pieces),
        [pltpu.VMEM((tokens, width), F32)] + blocks_shape(stride),
        12, 8 * slots * tokens * width, 4 * slots * width + 6 * tokens * width,
        in_specs=[VMEM] * (pieces + 4),
        out_specs=[VMEM] * (1 + pieces),
    )(*in_vmem(returned + [place, flip]), gate_values.T, readout)
    cot_own = exchange(cots)
    joined = cot_own
    if pairs_of is not None:
        joined = [
            call(
                functools.partial(join_kernel, capacity),
                pltpu.VMEM((len(pair) * capacity, width), BF16),
                2, 1, 4 * len(pair) * stride * width,
                in_specs=[VMEM] * len(pair),
                out_specs=VMEM,
            )(*in_vmem([cot_own[e] for e in pair]))
            for pair in pairs_of
        ]
    cot_far = forward(joined, far_mask)

    flops = 2 * slots * width * hidden + 4 * slots * parts * part * hidden
    both_t = pltpu.VMEM((parts * part, 2 * slots), BF16)
    square, acc, input_grad = call(
        functools.partial(
            grad_own_kernel, order, capacity, stride, tile, pieces, len(x0), parts, part
        ),
        [
            pltpu.VMEM((8, 128), F32),
            pltpu.VMEM((parts * part, hidden), F32),
            pltpu.HBM((tokens, width), F32),
        ],
        16, flops, 2 * width * hidden,
        in_specs=[VMEM] * (pieces + 2 * len(x0) + 3),
        out_specs=[VMEM, VMEM, ANY],
        scratch_shapes=[
            pltpu.VMEM((slots, width), BF16), both_t, pltpu.SemaphoreType.DMA
        ],
    )(*in_vmem(in_order(cot_own, order) + scaled0 + pc0 + [own_t, weights[0], input_grad]))
    far_square = shift(square, "rep", far_mask)
    pre_grad, far_rows, *sent = call(
        functools.partial(
            grad_far_kernel, experts, capacity, stride, tile, len(cot_far), parts, part
        ),
        [pltpu.VMEM((slots, hidden), BF16), both_t]
        + [pltpu.VMEM((part, hidden), BF16)] * (parts - 1),
        16, flops, 2 * width * hidden,
        in_specs=[VMEM] * (len(cot_far) + 5),
        out_specs=[VMEM] * (1 + parts),
        scratch_shapes=[pltpu.VMEM((slots, width), BF16)],
    )(*in_vmem(cot_far + [far_t, weights[0], scaled1, pc1, acc]))
    kept, square = call(
        functools.partial(grad_keep_kernel, part, tile),
        [pltpu.VMEM((part, hidden), F32), pltpu.VMEM((8, 128), F32)],
        12, 4 * slots * part * hidden, 2 * part * hidden,
        in_specs=[VMEM] * 6,
        out_specs=[VMEM] * 2,
    )(*in_vmem([far_rows, scaled1, pre_grad, acc, square, far_square]))
    came = [shift(sent[p - 1], "rep", p) for p in range(1, parts)]
    terms = [kept] + came
    squares = [square] + [shift(square, "rep", p) for p in range(1, parts)]
    grad_up, penalty = call(
        functools.partial(sum_kernel, 1.0 / (2.0 * tokens * groups * copies * width), parts),
        [jax.ShapeDtypeStruct((part, hidden), BF16), jax.ShapeDtypeStruct((1, 1), F32)],
        8, part * hidden, 8 * part * hidden,
        in_specs=[VMEM] * (2 * parts),
        out_specs=[VMEM, SMEM],
    )(*in_vmem(terms + squares))
    return grad_up[None], input_grad, penalty[0, 0]


def solution(mesh):
    both = P(("expert", "rep"), None)
    return jax.shard_map(
        body,
        mesh=mesh,
        in_specs=(both, both, P("expert", None, None), P("expert", None, None), both, both),
        out_specs=(P("expert", "rep", None), both, P()),
        check_vma=False,
    )
```
